32 devices in a mesh: dp: 8 (over y, x, core), mp: 4 (over z).
Axes of the slice: x: 2, y: 2, z: 4, core: 2. Of those that a mesh axis runs over, the one named last changes fastest.
Arguments:
- tokens: bfloat16 [12288, 4096], P('dp'), may hold values from -40 to 40
- norm_gain: bfloat16 [4096], replicated, may hold values from 0.099609375 to 1.8984375
- w_query: bfloat16 [4096, 2048], P(None, 'mp'), may hold values from -1 to 1
- w_key: bfloat16 [4096, 512], P(None, 'mp'), may hold values from -4 to 4
- w_value: bfloat16 [4096, 512], P(None, 'mp'), may hold values from -0.09375 to 0.09375
- w_out: bfloat16 [2048, 4096], P('mp'), may hold values from -0.125 to 0.125
- seq_starts: int32 [64], P('dp'), may hold values from 0 to 1408, as said below
- seq_lengths: int32 [64], P('dp'), may hold values from 128 to 640
- episode_ids: int32 [64], replicated, may hold values from 0 to 0, as said below
- class_ids: int32 [64], replicated, may hold values from 0 to 31
- query_flags: int32 [64], replicated, may hold values from 0 to 1
Outputs:
- log_probs: float32 [64, 32], P('dp')
- prototypes: float32 [32, 4096], P(None, 'mp')
The draws below stay inside these ranges and needn't reach their ends.
Inputs may be any that keep to these rules, and one draw needn't show every extreme that they name: `seq_starts`: slot s lies in the buffer of dp index s // 8; the slots of one buffer are disjoint and in increasing order of start; start plus length is at most 1536, and in every draw the last slot of some buffer ends at row 1536. `episode_ids`: every class of every episode has at least one support sequence.
All inputs are finite; a program needn't handle non-finite values.
Results may differ from the reference program's by a relative error of at most 0.004.
Values sent between devices are 32-bit elements; how exact they have to be, the bound alone decides.
No kernel may reach another device: no remote copies, remote signals or barrier semaphores. Data moves between devices by JAX's collectives and lax.ppermute only.
A program may use at most 128 MiB of HBM per device.

```python
import math
import jax
import jax.numpy as jnp
from jax import lax

D = 4096
HEAD_DIM = 128
HEADS = 16
KV_HEADS = 4
WAYS = 32
MIN_LEN = 128
SEQ_DEV = 8
CAP = 1536
NSEQ = 64
EPISODES = 1
CLASSES = 32


def packing(key):
    groups = NSEQ // SEQ_DEV
    subkeys = jax.random.split(jax.random.fold_in(key, 13), 4)
    spare_tokens = CAP - SEQ_DEV * MIN_LEN
    filled = jax.random.randint(subkeys[0], (groups,), 0, spare_tokens + 1)
    fullest = jax.random.randint(subkeys[1], (), 0, groups)
    filled = jnp.where(jnp.arange(groups) == fullest, spare_tokens, filled)
    raw_weights = jax.random.randint(subkeys[2], (groups, 2 * SEQ_DEV), 1, 17)
    weights = raw_weights * raw_weights * raw_weights
    shares = filled[:, None] * weights // jnp.sum(weights, axis=1, keepdims=True)
    remain = filled - jnp.sum(shares, axis=1)
    shares = shares.at[:, 0].add(remain)
    longest_slot = jax.random.randint(subkeys[3], (), 0, SEQ_DEV)
    single = jnp.where(jnp.arange(2 * SEQ_DEV) == longest_slot, spare_tokens, 0)
    shares = jnp.where((jnp.arange(groups) == fullest)[:, None], single[None, :], shares)
    lengths = MIN_LEN + shares[:, :SEQ_DEV]
    gap_sizes = shares[:, SEQ_DEV:]
    extents = lengths + gap_sizes
    starts = jnp.cumsum(extents, axis=1) - extents + gap_sizes
    return (starts.reshape(-1).astype(jnp.int32), lengths.reshape(-1).astype(jnp.int32))


def draw_seq_starts(key, part):
    return packing(key)[0]


def draw_seq_lengths(key, part):
    return packing(key)[1]


def labels(key):
    subkeys = jax.random.split(jax.random.fold_in(key, 7), 3)
    slot_index = jnp.arange(NSEQ, dtype=jnp.int32)
    extra_class = jax.random.randint(subkeys[0], (NSEQ,), 0, CLASSES)
    global_class = jnp.where(slot_index < CLASSES, slot_index, extra_class)
    coin = jax.random.randint(subkeys[1], (NSEQ,), 0, 2)
    asked_flag = jnp.where(slot_index < CLASSES, 0, jnp.where(slot_index == CLASSES, 1, coin))
    shuffle = jax.random.permutation(subkeys[2], NSEQ)
    return (global_class[shuffle], asked_flag[shuffle])


def draw_episode_ids(key, part):
    return (labels(key)[0] // WAYS).astype(jnp.int32)


def draw_class_ids(key, part):
    return (labels(key)[0] % WAYS).astype(jnp.int32)


def draw_query_flags(key, part):
    return labels(key)[1].astype(jnp.int32)


def query_key_pair(key):
    subkeys = jax.random.split(jax.random.fold_in(key, 21), 2)
    query_weight = jax.random.normal(subkeys[0], (D, HEADS * HEAD_DIM), jnp.float32) / math.sqrt(D)
    key_weight = jax.random.normal(subkeys[1], (D, KV_HEADS * HEAD_DIM), jnp.float32) / math.sqrt(D)
    return (jnp.clip(query_weight, -1.0, 1.0), jnp.clip(key_weight, -4.0, 4.0))


def draw_w_query(key, part):
    return query_key_pair(key)[0].astype(jnp.bfloat16)


def draw_w_key(key, part):
    return query_key_pair(key)[1].astype(jnp.bfloat16)


def draw_tokens(key, part):
    row_total = NSEQ // SEQ_DEV * CAP
    subkeys = jax.random.split(jax.random.fold_in(key, 31), 1)
    values = jax.random.normal(subkeys[0], (row_total, D), jnp.float32)
    values = jnp.clip(values, -6.0, 6.0)
    return values.astype(jnp.bfloat16)


def levels(own_key, shape, pieces, smallest, largest):
    level, own = 1.0, jax.random.fold_in(own_key, 6)
    for dim, parts in pieces:
        draws = jnp.exp(jax.random.uniform(jax.random.fold_in(own, dim), (parts,), jnp.float32, smallest / len(pieces), largest / len(pieces)))
        level = level * jnp.repeat(draws, shape[dim] // parts).reshape([-1 if axis == dim else 1 for axis in range(len(shape))])
    return level


def gaussian(key, shape, spread, most, shards=(), kind=jnp.bfloat16):
    entries = spread * jax.random.normal(key, shape, jnp.float32)
    if shards:
        entries = entries * levels(key, shape, shards, -0.22, 0.18)
    return jnp.clip(entries, -most, most).astype(kind)


def setup_inputs(seed: int = 0) -> dict:
    seeds = jax.random.split(jax.random.key(seed), 12)
    return {
        "tokens": draw_tokens(jax.random.fold_in(seeds[11], 71), 0),
        "norm_gain": jnp.clip(1.0 + 0.18 * jax.random.normal(seeds[1], (D,), jnp.float32), 0.099609375, 1.8984375).astype(jnp.bfloat16),
        "w_query": draw_w_query(jax.random.fold_in(seeds[11], 71), 0),
        "w_key": draw_w_key(jax.random.fold_in(seeds[11], 71), 0),
        "w_value": gaussian(seeds[4], (D, KV_HEADS * HEAD_DIM), D ** -0.5, 0.09375, ((1, 4),)),
        "w_out": gaussian(seeds[5], (HEADS * HEAD_DIM, D), (HEADS * HEAD_DIM) ** -0.5, 0.125, ((0, 4),)),
        "seq_starts": draw_seq_starts(jax.random.fold_in(seeds[11], 71), 0),
        "seq_lengths": draw_seq_lengths(jax.random.fold_in(seeds[11], 71), 0),
        "episode_ids": draw_episode_ids(jax.random.fold_in(seeds[11], 71), 0),
        "class_ids": draw_class_ids(jax.random.fold_in(seeds[11], 71), 0),
        "query_flags": draw_query_flags(jax.random.fold_in(seeds[11], 71), 0),
    }


ROPE_BASE = 500000.0
NEG_FILL = -1e+30

def rotate(vectors, positions):
    half_dim = vectors.shape[-1] // 2
    frequency = jnp.power(ROPE_BASE, -(jnp.arange(half_dim, dtype=jnp.float32) * 2.0 / vectors.shape[-1]))
    angles = positions.astype(jnp.float32)[:, None] * frequency[None, :]
    cosine = jnp.cos(angles)[:, None, :]
    sine_part = jnp.sin(angles)[:, None, :]
    leading = vectors[..., :half_dim]
    trailing = vectors[..., half_dim:]
    return jnp.concatenate([leading * cosine - trailing * sine_part, trailing * cosine + leading * sine_part], axis=-1)

def layout_of(starts, lengths, buffer_len):
    token_index = jnp.arange(buffer_len, dtype=jnp.int32)
    inside = (token_index[:, None] >= starts[None, :]) & (token_index[:, None] < (starts + lengths)[None, :])
    slot_number = jnp.arange(starts.shape[0], dtype=jnp.int32)
    segment = lax.optimization_barrier(jnp.sum(jnp.where(inside, slot_number[None, :] + 1, 0), axis=1)).astype(jnp.int32) - 1
    position = lax.optimization_barrier(jnp.sum(jnp.where(inside, token_index[:, None] - starts[None, :], 0), axis=1)).astype(jnp.int32)
    return (segment, position, inside)

def allowed_mask(segment, row_start, row_count, col_count):
    rows_index = row_start + jnp.arange(row_count, dtype=jnp.int32)
    cols_index = jnp.arange(col_count, dtype=jnp.int32)
    seg_rows = segment[row_start:row_start + row_count]
    seg_cols = segment[:col_count]
    same = (seg_rows[:, None] == seg_cols[None, :]) & (seg_rows[:, None] >= 0) & (cols_index[None, :] < rows_index[:, None])
    return (rows_index[:, None] == cols_index[None, :]) | same

def softmax_rows(scores, permitted):
    masked_scores = jnp.where(permitted[None, None], scores, NEG_FILL)
    row_peak = lax.optimization_barrier(jnp.max(masked_scores, axis=-1, keepdims=True))
    exponent = jnp.exp(masked_scores - row_peak)
    totals = lax.optimization_barrier(jnp.sum(exponent, axis=-1, keepdims=True))
    return (exponent / totals).astype(jnp.bfloat16)

def reference(tokens, norm_gain, w_query, w_key, w_value, w_out, seq_starts, seq_lengths, episode_ids, class_ids, query_flags):
    group_count = NSEQ // SEQ_DEV
    group_size = HEADS // KV_HEADS
    inv_root = 1.0 / math.sqrt(HEAD_DIM)
    highest = lax.Precision.HIGHEST

    def embed_group(row_items):
        buffer_rows, starts, lengths = row_items
        segment, position, inside = layout_of(starts, lengths, CAP)
        widened = buffer_rows.astype(jnp.float32)
        normed = (widened * lax.rsqrt(lax.optimization_barrier(jnp.mean(widened * widened, axis=-1, keepdims=True)) + 1e-05) * norm_gain.astype(jnp.float32)).astype(jnp.bfloat16)
        queries = rotate(jnp.dot(normed, w_query, preferred_element_type=jnp.float32).reshape(CAP, HEADS, HEAD_DIM), position).astype(jnp.bfloat16)
        queries = queries.reshape(CAP, KV_HEADS, group_size, HEAD_DIM)
        keys_rot = rotate(jnp.dot(normed, w_key, preferred_element_type=jnp.float32).reshape(CAP, KV_HEADS, HEAD_DIM), position).astype(jnp.bfloat16)
        values_all = jnp.dot(normed, w_value, preferred_element_type=jnp.float32).astype(jnp.bfloat16).reshape(CAP, KV_HEADS, HEAD_DIM)
        scores = jnp.einsum('qngd,knd->ngqk', queries.astype(jnp.float32), keys_rot.astype(jnp.float32), precision=highest) * inv_root
        permitted = allowed_mask(segment, 0, CAP, CAP)
        attention_probs = softmax_rows(scores, permitted)
        attended = jnp.einsum('ngqk,knd->qngd', attention_probs.astype(jnp.float32), values_all.astype(jnp.float32), precision=highest)
        attended = attended.astype(jnp.bfloat16).reshape(CAP, HEADS * HEAD_DIM)
        layer_out = widened + jnp.dot(attended, w_out, preferred_element_type=jnp.float32)
        member = inside.T.astype(jnp.float32)
        return jnp.dot(member, layer_out, precision=highest) / lengths.astype(jnp.float32)[:, None]
    pooled = lax.map(embed_group, (tokens.reshape(group_count, CAP, D), seq_starts.reshape(group_count, SEQ_DEV), seq_lengths.reshape(group_count, SEQ_DEV)))
    pooled = pooled.reshape(NSEQ, D)
    embedded = pooled * lax.rsqrt(lax.optimization_barrier(jnp.mean(pooled * pooled, axis=-1, keepdims=True)) + 1e-06)
    global_class = episode_ids * WAYS + class_ids
    is_support = query_flags == 0
    select_all = ((global_class[None, :] == jnp.arange(CLASSES, dtype=jnp.int32)[:, None]) & is_support[None, :]).astype(jnp.float32)
    class_sums = jnp.dot(select_all, embedded, precision=highest)
    prototypes = class_sums * lax.rsqrt(lax.optimization_barrier(jnp.mean(class_sums * class_sums, axis=-1, keepdims=True)) + 1e-06)
    episode_protos = prototypes.reshape(EPISODES, WAYS, D)

    def score_row(row_items):
        vector, episode = row_items
        chosen = lax.dynamic_index_in_dim(episode_protos, episode, 0, keepdims=False)
        difference = vector[None, :] - chosen
        return lax.optimization_barrier(jnp.sum(difference * difference, axis=-1))
    distance = lax.map(score_row, (embedded, episode_ids))
    logits = -distance / math.sqrt(D)
    row_peak = lax.optimization_barrier(jnp.max(logits, axis=-1, keepdims=True))
    shifted = logits - row_peak
    log_probs = shifted - jnp.log(lax.optimization_barrier(jnp.sum(jnp.exp(shifted), axis=-1, keepdims=True)))
    log_probs = jnp.where(query_flags[:, None] == 1, log_probs, 0.0)
    return (log_probs, prototypes)
```

```python
import functools
import math

import jax
import jax.numpy as jnp
import numpy as np
from jax import lax
from jax.experimental import pallas as pl
from jax.experimental.pallas import tpu as pltpu
from jax.sharding import PartitionSpec as P

HEAD_DIM = 128
WAYS = 32
MAX_LEN = 640
ROPE_BASE = 500000.0
NEG_FILL = -1e30
ROWS = 256
QBLOCK = 128

HIGHEST = lax.Precision.HIGHEST
VMEM = pltpu.VMEM


def rope_tables(rows):
    half = HEAD_DIM // 2
    freq = ROPE_BASE ** (-(np.arange(half) * 2.0 / HEAD_DIM))
    angle = np.arange(rows)[:, None] * freq[None, :]
    cosine = np.concatenate([np.cos(angle), np.cos(angle)], axis=1)
    sine = np.concatenate([-np.sin(angle), np.sin(angle)], axis=1)
    return cosine.astype(np.float32), sine.astype(np.float32)


def layer_kernel(
    mp_size,
    rank_ref,
    starts_ref,
    lengths_ref,
    tokens_hbm,
    gain_ref,
    wq_hbm,
    wk_hbm,
    wv_hbm,
    wo_hbm,
    cos_hbm,
    sin_hbm,
    *rest,
):
    outs = rest[:mp_size]
    (
        x_s, w_s, wo_s, cos_s, sin_s, raw_a, raw_b, inv_s,
        q_s, k_s, v_s, srow_s, tok_s, wacc_s, hp_s, xsem, wsem,
    ) = rest[mp_size:]
    buffer_len, width = x_s.shape
    q_cols = wq_hbm.shape[1]
    heads = q_cols // HEAD_DIM
    blocks = buffer_len // ROWS
    slots = starts_ref.shape[0]
    share = width // mp_size
    rank = rank_ref[0]

    def x_copy(i):
        rows = pl.ds(i * ROWS, ROWS)
        return pltpu.make_async_copy(tokens_hbm.at[rows], x_s.at[rows], xsem.at[i])

    weight_copies = [
        pltpu.make_async_copy(wq_hbm, w_s.at[:, pl.ds(0, q_cols)], wsem.at[0]),
        pltpu.make_async_copy(wk_hbm, w_s.at[:, pl.ds(q_cols, HEAD_DIM)], wsem.at[1]),
        pltpu.make_async_copy(
            wv_hbm, w_s.at[:, pl.ds(q_cols + HEAD_DIM, HEAD_DIM)], wsem.at[2]
        ),
        pltpu.make_async_copy(cos_hbm, cos_s, wsem.at[3]),
        pltpu.make_async_copy(sin_hbm, sin_s, wsem.at[4]),
        pltpu.make_async_copy(wo_hbm, wo_s, wsem.at[5]),
    ]
    x_copy(0).start()
    for c in weight_copies[:3]:
        c.start()
    x_copy(1).start()
    for c in weight_copies[3:5]:
        c.start()
    for i in range(2, blocks):
        x_copy(i).start()
    weight_copies[5].start()

    def first_rows(i, _):
        row = i * QBLOCK + lax.broadcasted_iota(jnp.int32, (QBLOCK, HEAD_DIM), 0)
        first = row
        for s in range(slots):
            begin = starts_ref[s]
            inside = (row >= begin) & (row < begin + lengths_ref[s])
            first = jnp.where(inside, begin, first)
        srow_s[pl.ds(pl.multiple_of(i * QBLOCK, QBLOCK), QBLOCK), :] = first
        return 0

    lax.fori_loop(0, buffer_len // QBLOCK, first_rows, 0)
    tok_s[...] = jnp.zeros_like(tok_s)
    wacc_s[...] = jnp.zeros_like(wacc_s)

    def members(row_first, count, sublanes):
        row = row_first + lax.broadcasted_iota(jnp.int32, (sublanes, count), 1)
        slot = lax.broadcasted_iota(jnp.int32, (sublanes, count), 0)
        low = jnp.zeros((sublanes, count), jnp.int32)
        high = jnp.zeros((sublanes, count), jnp.int32)
        for s in range(slots):
            low = jnp.where(slot == s, starts_ref[s], low)
            high = jnp.where(slot == s, starts_ref[s] + lengths_ref[s], high)
        return jnp.where((row >= low) & (row < high), 1.0, 0.0)

    share_cols = pl.ds(pl.multiple_of(rank * share, share), share)
    score_scale = math.log2(math.e) / math.sqrt(HEAD_DIM)

    def project(i, raw, parity):
        rows = pl.ds(pl.multiple_of(i * ROWS, ROWS), ROWS)
        x = x_s[rows, :]
        scaled = x * gain_ref[...]
        raw[...] = jnp.dot(scaled, w_s[...], preferred_element_type=jnp.float32)
        wide = x.astype(jnp.float32)
        square = jnp.sum(wide * wide, axis=1, keepdims=True)
        inv = lax.rsqrt(square * (1.0 / width) + 1e-05)
        inv_s[parity] = jnp.broadcast_to(inv, (ROWS, HEAD_DIM))
        member = members(i * ROWS, ROWS, 16).astype(jnp.bfloat16)
        tok_s[...] += jnp.dot(
            member, x_s[rows, share_cols], preferred_element_type=jnp.float32
        )

    def finish(i, raw, parity):
        source = pl.ds(pl.multiple_of(jnp.maximum(i, 0) * ROWS, ROWS), ROWS)
        inv = inv_s[parity]
        cosine = cos_s[source, :] * inv
        sine = sin_s[source, :] * inv
        target = pl.ds(pl.multiple_of((i + 1) * ROWS, ROWS), ROWS)
        q_cosine = cosine * score_scale
        q_sine = sine * score_scale
        for h in range(heads):
            head = raw[:, h * HEAD_DIM : (h + 1) * HEAD_DIM]
            turned = head * q_cosine + pltpu.roll(head, HEAD_DIM // 2, 1) * q_sine
            q_s[h, target, :] = turned.astype(jnp.bfloat16)
        key = raw[:, q_cols : q_cols + HEAD_DIM]
        turned = key * cosine + pltpu.roll(key, HEAD_DIM // 2, 1) * sine
        k_s[target, :] = turned.astype(jnp.bfloat16)
        value = raw[:, q_cols + HEAD_DIM :] * inv
        v_s[target, :] = value.astype(jnp.bfloat16)

    for c in weight_copies[:5]:
        c.wait()

    def pair(j, _):
        x_copy(2 * j).wait()
        project(2 * j, raw_a, 0)
        finish(2 * j - 1, raw_b, 1)
        x_copy(2 * j + 1).wait()
        project(2 * j + 1, raw_b, 1)
        finish(2 * j, raw_a, 0)
        return 0

    lax.fori_loop(0, blocks // 2, pair, 0)
    finish(blocks - 1, raw_b, 1)

    most = (MAX_LEN - 1 + QBLOCK - 1) // QBLOCK + 1

    def attend(i, _):
        top = i * QBLOCK
        lowest = top
        for s in range(slots):
            begin = starts_ref[s]
            inside = (top >= begin) & (top < begin + lengths_ref[s])
            lowest = jnp.where(inside, begin, lowest)
        count = i - lowest // QBLOCK + 1
        for n in range(1, most + 1):

            @pl.when(count == n)
            def _(n=n):
                keys = n * QBLOCK
                key_first = pl.multiple_of((i + 1 - n) * QBLOCK, QBLOCK)
                q_rows = pl.ds(pl.multiple_of(ROWS + top, QBLOCK), QBLOCK)
                key_block = k_s[pl.ds(pl.multiple_of(ROWS + key_first, QBLOCK), keys), :]
                first = srow_s[pl.ds(pl.multiple_of(top, QBLOCK), QBLOCK), :]
                row = top + lax.broadcasted_iota(jnp.int32, (QBLOCK, keys), 0)
                col = key_first + lax.broadcasted_iota(jnp.int32, (QBLOCK, keys), 1)
                first = jnp.concatenate([first] * n, axis=1)
                permitted = (col >= first) & (col <= row)
                for h in range(heads):
                    score = lax.dot_general(
                        q_s[h, q_rows, :],
                        key_block,
                        (((1,), (1,)), ((), ())),
                        preferred_element_type=jnp.float32,
                    )
                    score = jnp.where(permitted, score, NEG_FILL)
                    peak = jnp.max(score, axis=1, keepdims=True)
                    power = jnp.exp2(score - peak)
                    total = jnp.sum(power, axis=1, keepdims=True)
                    share_of = power * (1.0 / total)
                    wacc_s[h : h + 1, pl.ds(key_first, keys)] += jnp.sum(
                        share_of, axis=0, keepdims=True
                    )

        return 0

    lax.fori_loop(0, buffer_len // QBLOCK, attend, 0)

    member = members(0, buffer_len, 8)
    weighted = jnp.concatenate([member * wacc_s[h : h + 1, :] for h in range(heads)], axis=0)
    count = heads * 8
    high = weighted.astype(jnp.bfloat16)
    low = (weighted - high.astype(jnp.float32)).astype(jnp.bfloat16)
    both = jnp.dot(
        jnp.concatenate([high, low], axis=0),
        v_s[pl.ds(ROWS, buffer_len), :],
        preferred_element_type=jnp.float32,
    )
    sums = both[:count] + both[count:]
    sums = jnp.concatenate([sums[h * 8 : (h + 1) * 8] for h in range(heads)], axis=1)
    high = sums.astype(jnp.bfloat16)
    low = (sums - high.astype(jnp.float32)).astype(jnp.bfloat16)
    weight_copies[5].wait()
    parts = jnp.dot(
        jnp.concatenate([high, low], axis=0), wo_s[...], preferred_element_type=jnp.float32
    )
    hp_s[...] = parts[:8] + parts[8:]
    outs[0][...] = hp_s[:, share_cols] + tok_s[0:8, :]
    for k in range(1, mp_size):
        other = lax.rem(rank + k, mp_size)
        outs[k][...] = hp_s[:, pl.ds(pl.multiple_of(other * share, share), share)]


def layer_call(mp_size, rank, starts, lengths, tokens, gain, wq, wk, wv, wo):
    buffer_len, width = tokens.shape
    slots = starts.shape[0]
    assert slots == 8 and wk.shape[1] == HEAD_DIM
    heads = wq.shape[1] // HEAD_DIM
    columns = wq.shape[1] + 2 * HEAD_DIM
    blocks = buffer_len // ROWS
    assert blocks % 2 == 0
    share = width // mp_size
    cosine, sine = rope_tables(buffer_len)
    smem = pl.BlockSpec(memory_space=pltpu.SMEM)
    vmem = pl.BlockSpec(memory_space=VMEM)
    hbm = pl.BlockSpec(memory_space=pl.ANY)
    f32, bf16 = jnp.float32, jnp.bfloat16
    padded = buffer_len + ROWS
    return pl.pallas_call(
        functools.partial(layer_kernel, mp_size),
        out_shape=[jax.ShapeDtypeStruct((slots, share), f32)] * mp_size,
        in_specs=[smem, smem, smem, hbm, vmem, hbm, hbm, hbm, hbm, hbm, hbm],
        out_specs=[vmem] * mp_size,
        scratch_shapes=[
            VMEM((buffer_len, width), bf16),
            VMEM((width, columns), bf16),
            VMEM(wo.shape, bf16),
            VMEM((buffer_len, HEAD_DIM), f32),
            VMEM((buffer_len, HEAD_DIM), f32),
            VMEM((ROWS, columns), f32),
            VMEM((ROWS, columns), f32),
            VMEM((2, ROWS, HEAD_DIM), f32),
            VMEM((heads, padded, HEAD_DIM), bf16),
            VMEM((padded, HEAD_DIM), bf16),
            VMEM((padded, HEAD_DIM), bf16),
            VMEM((buffer_len, HEAD_DIM), jnp.int32),
            VMEM((16, share), f32),
            VMEM((8, buffer_len), f32),
            VMEM((slots, width), f32),
            pltpu.SemaphoreType.DMA((blocks,)),
            pltpu.SemaphoreType.DMA((6,)),
        ],
        compiler_params=pltpu.CompilerParams(vmem_limit_bytes=60 * 1024 * 1024),
        name="layer",
    )(rank, starts, lengths, tokens, gain, wq, wk, wv, wo, jnp.asarray(cosine), jnp.asarray(sine))


def gram_kernel(dp_size, rank_ref, *rest):
    parts, (all_ref, gram_ref) = rest[:dp_size], rest[dp_size:]
    rank = rank_ref[0]
    rows = parts[0].shape[0]
    for k in range(dp_size):
        owner = lax.rem(rank + dp_size - k, dp_size)
        all_ref[pl.ds(pl.multiple_of(owner * rows, rows), rows), :] = parts[k][...]
    pooled = all_ref[...]
    gram_ref[...] = lax.dot_general(
        pooled, pooled, (((1,), (1,)), ((), ())), precision=HIGHEST,
        preferred_element_type=jnp.float32,
    )


def score_kernel(mp_size, width, episodes, rank_ref, *rest):
    grams = rest[:mp_size]
    all_ref, ids_ref, own_ref, log_ref, proto_ref, gram_s, cross_s = rest[mp_size:]
    rank = rank_ref[0]
    total = all_ref.shape[0]
    own_count = log_ref.shape[0]
    classes = episodes * WAYS
    gram = grams[0][...]
    for k in range(1, mp_size):
        gram = gram + grams[k][...]
    gram_s[...] = gram
    eye = lax.broadcasted_iota(jnp.int32, (total, total), 0) == lax.broadcasted_iota(
        jnp.int32, (total, total), 1
    )
    square = jnp.sum(jnp.where(eye, gram, 0.0), axis=1, keepdims=True)
    scale = lax.rsqrt(square * (1.0 / width) + 1e-06)
    label = jnp.max(jnp.where(eye, ids_ref[...], -1), axis=1, keepdims=True)
    class_of = lax.broadcasted_iota(jnp.int32, (total, classes), 1)
    select = jnp.where(label == class_of, scale, 0.0)
    cross = jnp.dot(gram, select, precision=HIGHEST, preferred_element_type=jnp.float32)
    norm = jnp.maximum(jnp.sum(cross * select, axis=0, keepdims=True), 0.0)
    proto_scale = lax.rsqrt(norm * (1.0 / width) + 1e-06)
    proto_ref[...] = lax.dot_general(
        select * proto_scale, all_ref[...], (((0,), (0,)), ((), ())), precision=HIGHEST,
        preferred_element_type=jnp.float32,
    )
    cross_s[...] = (
        square * scale * scale
        + norm * proto_scale * proto_scale
        - 2.0 * (scale * proto_scale) * cross
    )
    distance = cross_s[pl.ds(pl.multiple_of(rank * own_count, own_count), own_count), :]
    own_episode = own_ref[:, 0:1]
    own_query = own_ref[:, 1:2]
    picked = distance[:, :WAYS]
    for e in range(1, episodes):
        picked = jnp.where(own_episode == e, distance[:, e * WAYS : (e + 1) * WAYS], picked)
    logits = picked * (-1.0 / math.sqrt(width))
    peak = jnp.max(logits, axis=1, keepdims=True)
    shifted = logits - peak
    out = shifted - jnp.log(jnp.sum(jnp.exp(shifted), axis=1, keepdims=True))
    log_ref[...] = jnp.where(own_query == 1, out, 0.0)


def shifted_by(axis, size, k):
    return [(i, (i + k) % size) for i in range(size)]


def per_device(
    tokens, norm_gain, w_query, w_key, w_value, w_out,
    seq_starts, seq_lengths, episode_ids, class_ids, query_flags,
):
    width = tokens.shape[1]
    slots = seq_starts.shape[0]
    total = episode_ids.shape[0]
    episodes = max(1, total // (2 * WAYS))
    mp_size = lax.axis_size("mp")
    dp_size = lax.axis_size("dp")
    mp_rank = lax.axis_index("mp")
    dp_rank = lax.axis_index("dp")
    share = width // mp_size
    f32 = jnp.float32
    vmem = pl.BlockSpec(memory_space=VMEM)
    smem = pl.BlockSpec(memory_space=pltpu.SMEM)

    parts = layer_call(
        mp_size, mp_rank.reshape(1), seq_starts, seq_lengths, tokens,
        norm_gain.reshape(1, width), w_query, w_key, w_value, w_out,
    )
    pooled = parts[0]
    arrived = [
        lax.ppermute(parts[k], "mp", shifted_by("mp", mp_size, k)) for k in range(1, mp_size)
    ]
    for a in arrived:
        pooled = pooled + a
    pooled = pooled / seq_lengths.astype(f32)[:, None]

    gathered = [pooled] + [
        lax.ppermute(pooled, "dp", shifted_by("dp", dp_size, k)) for k in range(1, dp_size)
    ]
    everyone, gram = pl.pallas_call(
        functools.partial(gram_kernel, dp_size),
        out_shape=[
            jax.ShapeDtypeStruct((total, share), f32),
            jax.ShapeDtypeStruct((total, total), f32),
        ],
        in_specs=[smem] + [vmem] * dp_size,
        out_specs=[vmem, vmem],
        name="gram",
    )(dp_rank.reshape(1), *gathered)

    grams = [gram] + [
        lax.ppermute(gram, "mp", shifted_by("mp", mp_size, k)) for k in range(1, mp_size)
    ]
    ids = jnp.where(query_flags == 0, episode_ids * WAYS + class_ids, -1).reshape(1, total)
    own_first = dp_rank * slots
    own = jnp.stack(
        [
            lax.dynamic_slice_in_dim(episode_ids, own_first, slots, 0),
            lax.dynamic_slice_in_dim(query_flags, own_first, slots, 0),
        ],
        axis=1,
    )
    log_probs, prototypes = pl.pallas_call(
        functools.partial(score_kernel, mp_size, width, episodes),
        out_shape=[
            jax.ShapeDtypeStruct((slots, WAYS), f32),
            jax.ShapeDtypeStruct((episodes * WAYS, share), f32),
        ],
        in_specs=[smem] + [vmem] * (mp_size + 3),
        out_specs=[vmem, vmem],
        scratch_shapes=[VMEM((total, total), f32), VMEM((total, episodes * WAYS), f32)],
        name="score",
    )(dp_rank.reshape(1), *grams, everyone, ids, own)
    return log_probs, prototypes


def solution(mesh):
    placed = (
        P("dp", None), P(), P(None, "mp"), P(None, "mp"), P(None, "mp"), P("mp", None),
        P("dp"), P("dp"), P(), P(), P(),
    )
    return jax.shard_map(
        per_device,
        mesh=mesh,
        in_specs=placed,
        out_specs=(P("dp", None), P(None, "mp")),
        check_vma=False,
    )
```

```python
import functools
import math

import jax
import jax.numpy as jnp
import numpy as np
from jax import lax
from jax.experimental import pallas as pl
from jax.experimental.pallas import tpu as pltpu
from jax.sharding import PartitionSpec as P

HEAD_DIM = 128
WAYS = 32
MAX_LEN = 640
ROPE_BASE = 500000.0
NEG_FILL = -1e30
ROWS = 512
QBLOCK = 128
AROWS = 256
CHUNKS = 4
LAYER_VMEM = 56 * 1024 * 1024
SMALL_VMEM = 8 * 1024 * 1024

HIGHEST = lax.Precision.HIGHEST
VMEM = pltpu.VMEM


def rope_tables(rows):
    half = HEAD_DIM // 2
    freq = ROPE_BASE ** (-(np.arange(half) * 2.0 / HEAD_DIM))
    angle = np.arange(rows)[:, None] * freq[None, :]
    cosine = np.concatenate([np.cos(angle), np.cos(angle)], axis=1)
    sine = np.concatenate([-np.sin(angle), np.sin(angle)], axis=1)
    return cosine.astype(np.float32), sine.astype(np.float32)


def layer_kernel(
    mp_size,
    rank_ref,
    starts_hbm,
    lengths_hbm,
    tokens_hbm,
    gain_hbm,
    wq_hbm,
    wk_hbm,
    wv_hbm,
    wo_hbm,
    cos_hbm,
    sin_hbm,
    *rest,
):
    outs = rest[:mp_size]
    (
        x_s, wq_s, wkv_s, wo_s, cos_s, sin_s, raw_q, raw_kv, square_s,
        q_s, k_s, v_s, srow_s, tok_s, wacc_s, hp_s, gain_s,
        gain_flat, starts_ref, lengths_ref, xsem, wsem, tsem,
    ) = rest[mp_size:]
    buffer_len, width = x_s.shape
    q_cols = wq_hbm.shape[1]
    heads = q_cols // HEAD_DIM
    blocks = buffer_len // ROWS
    slots = starts_hbm.shape[0]
    share = width // mp_size
    depth = width // CHUNKS
    rank = rank_ref[0]

    def x_copy(i):
        rows = pl.ds(i * ROWS, ROWS)
        return pltpu.make_async_copy(tokens_hbm.at[rows], x_s.at[rows], xsem.at[i - 1])

    def chunk_copies(c):
        part = pl.ds(pl.multiple_of(c * depth, depth), depth)
        rows = pl.ds(0, ROWS)
        return [
            pltpu.make_async_copy(
                tokens_hbm.at[rows, part], x_s.at[rows, part], wsem.at[c, 0]
            ),
            pltpu.make_async_copy(wq_hbm.at[part], wq_s.at[part], wsem.at[c, 1]),
            pltpu.make_async_copy(
                wk_hbm.at[part], wkv_s.at[part, pl.ds(0, HEAD_DIM)], wsem.at[c, 2]
            ),
            pltpu.make_async_copy(
                wv_hbm.at[part], wkv_s.at[part, pl.ds(HEAD_DIM, HEAD_DIM)], wsem.at[c, 3]
            ),
        ]

    table_copies = [
        pltpu.make_async_copy(cos_hbm, cos_s, tsem.at[0]),
        pltpu.make_async_copy(sin_hbm, sin_s, tsem.at[1]),
    ]
    out_copy = pltpu.make_async_copy(wo_hbm, wo_s, tsem.at[2])
    small_copies = [
        pltpu.make_async_copy(starts_hbm, starts_ref, tsem.at[3]),
        pltpu.make_async_copy(lengths_hbm, lengths_ref, tsem.at[4]),
        pltpu.make_async_copy(gain_hbm, gain_flat, tsem.at[5]),
    ]
    for copy in small_copies:
        copy.start()
    for c in range(CHUNKS):
        for copy in chunk_copies(c):
            copy.start()
    x_copy(1).start()
    for copy in table_copies:
        copy.start()
    for i in range(2, blocks):
        x_copy(i).start()
    out_copy.start()

    for copy in small_copies:
        copy.wait()

    def first_rows(i, _):
        row = i * QBLOCK + lax.broadcasted_iota(jnp.int32, (QBLOCK, HEAD_DIM), 0)
        first = row
        for s in range(slots):
            begin = starts_ref[s]
            inside = (row >= begin) & (row < begin + lengths_ref[s])
            first = jnp.where(inside, begin, first)
        srow_s[pl.ds(pl.multiple_of(i * QBLOCK, QBLOCK), QBLOCK), :] = first
        return 0

    lax.fori_loop(0, buffer_len // QBLOCK, first_rows, 0)
    gain_s[...] = gain_flat[...].reshape(1, width)
    tok_s[...] = jnp.zeros_like(tok_s)
    wacc_s[...] = jnp.zeros_like(wacc_s)
    raw_q[...] = jnp.zeros_like(raw_q)
    raw_kv[...] = jnp.zeros_like(raw_kv)
    square_s[...] = jnp.zeros_like(square_s)

    def members(row_first, count, sublanes):
        row = row_first + lax.broadcasted_iota(jnp.int32, (sublanes, count), 1)
        slot = lax.broadcasted_iota(jnp.int32, (sublanes, count), 0)
        low = jnp.zeros((sublanes, count), jnp.int32)
        high = jnp.zeros((sublanes, count), jnp.int32)
        for s in range(slots):
            low = jnp.where(slot == s, starts_ref[s], low)
            high = jnp.where(slot == s, starts_ref[s] + lengths_ref[s], high)
        return jnp.where((row >= low) & (row < high), 1.0, 0.0)

    share_cols = pl.ds(pl.multiple_of(rank * share, share), share)
    score_scale = math.log2(math.e) / math.sqrt(HEAD_DIM)
    half = ROWS // 2

    def dots(scaled, w_q, w_kv):
        f32 = jnp.float32
        return (
            jnp.dot(scaled, w_q, preferred_element_type=f32),
            jnp.dot(scaled[:half], w_kv, preferred_element_type=f32),
            jnp.dot(scaled[half:], w_kv, preferred_element_type=f32),
        )

    def lane_squares(x):
        wide = x.astype(jnp.float32)
        total = None
        for c in range(x.shape[1] // HEAD_DIM):
            piece = wide[:, c * HEAD_DIM : (c + 1) * HEAD_DIM]
            total = piece * piece if total is None else total + piece * piece
        return total

    def token_sums(i, rows):
        member = members(i * ROWS, ROWS, 16).astype(jnp.bfloat16)
        tok_s[...] += jnp.dot(
            member, x_s[rows, share_cols], preferred_element_type=jnp.float32
        )

    def first_chunk(c, _):
        for copy in chunk_copies(c):
            copy.wait()
        part = pl.ds(pl.multiple_of(c * depth, depth), depth)
        x = x_s[0:ROWS, part]
        q, kv_a, kv_b = dots(x * gain_s[:, part], wq_s[part, :], wkv_s[part, :])
        raw_q[...] += q
        raw_kv[0:half, :] += kv_a
        raw_kv[half:, :] += kv_b
        square_s[...] += lane_squares(x)
        return 0

    def project(i):
        rows = pl.ds(pl.multiple_of(i * ROWS, ROWS), ROWS)
        x = x_s[rows, :]
        q, kv_a, kv_b = dots(x * gain_s[...], wq_s[...], wkv_s[...])
        raw_q[...] = q
        raw_kv[0:half, :] = kv_a
        raw_kv[half:, :] = kv_b
        square_s[...] = lane_squares(x)
        token_sums(i, rows)

    def finish(i):
        rows = pl.ds(pl.multiple_of(i * ROWS, ROWS), ROWS)
        square = jnp.sum(square_s[...], axis=1, keepdims=True)
        inv = lax.rsqrt(square * (1.0 / width) + 1e-05)
        cosine = cos_s[rows, :] * inv
        sine = sin_s[rows, :] * inv
        q_cosine = cosine * score_scale
        q_sine = sine * score_scale
        for h in range(heads):
            head = raw_q[:, h * HEAD_DIM : (h + 1) * HEAD_DIM]
            turned = head * q_cosine + pltpu.roll(head, HEAD_DIM // 2, 1) * q_sine
            q_s[h, rows, :] = turned.astype(jnp.bfloat16)
        key = raw_kv[:, :HEAD_DIM]
        turned = key * cosine + pltpu.roll(key, HEAD_DIM // 2, 1) * sine
        k_s[rows, :] = turned.astype(jnp.bfloat16)
        v_s[rows, :] = (raw_kv[:, HEAD_DIM:] * inv).astype(jnp.bfloat16)

    lax.fori_loop(0, CHUNKS, first_chunk, 0)
    token_sums(0, pl.ds(0, ROWS))
    for copy in table_copies:
        copy.wait()

    def step(i, _):
        x_copy(i).wait()
        finish(i - 1)
        project(i)
        return 0

    lax.fori_loop(1, blocks, step, 0)
    finish(blocks - 1)

    most = (MAX_LEN - 1 + QBLOCK - 1) // QBLOCK
    parts_per = AROWS // QBLOCK

    def attend(i, _):
        top = i * AROWS
        lowest = top
        for s in range(slots):
            begin = starts_ref[s]
            inside = (top >= begin) & (top < begin + lengths_ref[s])
            lowest = jnp.where(inside, begin, lowest)
        ahead = i * parts_per - lowest // QBLOCK
        for n in range(most + 1):

            @pl.when(ahead == n)
            def _(n=n):
                for part in range(parts_per):
                    before = min(n + part, most)
                    keys = (before + 1) * QBLOCK
                    row_first = pl.multiple_of(top + part * QBLOCK, QBLOCK)
                    key_first = pl.multiple_of(row_first - before * QBLOCK, QBLOCK)
                    q_rows = pl.ds(row_first, QBLOCK)
                    key_block = k_s[pl.ds(key_first, keys), :]
                    first = srow_s[q_rows, :]
                    row = row_first + lax.broadcasted_iota(jnp.int32, (QBLOCK, keys), 0)
                    col = key_first + lax.broadcasted_iota(jnp.int32, (QBLOCK, keys), 1)
                    first = jnp.concatenate([first] * (before + 1), axis=1)
                    permitted = (col >= first) & (col <= row)
                    for h in range(heads):
                        score = lax.dot_general(
                            q_s[h, q_rows, :],
                            key_block,
                            (((1,), (1,)), ((), ())),
                            preferred_element_type=jnp.float32,
                        )
                        score = jnp.where(permitted, score, NEG_FILL)
                        peak = jnp.max(score, axis=1, keepdims=True)
                        power = jnp.exp2(score - peak)
                        total = jnp.sum(power, axis=1, keepdims=True)
                        share_of = power * (1.0 / total)
                        wacc_s[h : h + 1, pl.ds(key_first, keys)] += jnp.sum(
                            share_of, axis=0, keepdims=True
                        )

        return 0

    lax.fori_loop(0, buffer_len // AROWS, attend, 0)

    member = members(0, buffer_len, 8)
    weighted = jnp.concatenate([member * wacc_s[h : h + 1, :] for h in range(heads)], axis=0)
    count = heads * 8
    high = weighted.astype(jnp.bfloat16)
    low = (weighted - high.astype(jnp.float32)).astype(jnp.bfloat16)
    both = jnp.dot(
        jnp.concatenate([high, low], axis=0), v_s[...], preferred_element_type=jnp.float32
    )
    sums = both[:count] + both[count:]
    sums = jnp.concatenate([sums[h * 8 : (h + 1) * 8] for h in range(heads)], axis=1)
    high = sums.astype(jnp.bfloat16)
    low = (sums - high.astype(jnp.float32)).astype(jnp.bfloat16)
    out_copy.wait()
    parts = jnp.dot(
        jnp.concatenate([high, low], axis=0), wo_s[...], preferred_element_type=jnp.float32
    )
    slot = lax.broadcasted_iota(jnp.int32, (8, HEAD_DIM), 0)
    tokens_in = jnp.ones((8, HEAD_DIM), jnp.int32)
    for s in range(slots):
        tokens_in = jnp.where(slot == s, lengths_ref[s], tokens_in)
    per_token = (1.0 / tokens_in.astype(jnp.float32))[:, 0:1]
    hp_s[...] = (parts[:8] + parts[8:]) * per_token
    outs[0][...] = hp_s[:, share_cols] + tok_s[0:8, :] * per_token
    for k in range(1, mp_size):
        other = lax.rem(rank + k, mp_size)
        outs[k][...] = hp_s[:, pl.ds(pl.multiple_of(other * share, share), share)]


def layer_call(mp_size, rank, starts, lengths, tokens, gain, wq, wk, wv, wo):
    buffer_len, width = tokens.shape
    slots = starts.shape[0]
    assert slots == 8 and wk.shape[1] == HEAD_DIM
    heads = wq.shape[1] // HEAD_DIM
    blocks = buffer_len // ROWS
    share = width // mp_size
    cosine, sine = rope_tables(buffer_len)
    smem = pl.BlockSpec(memory_space=pltpu.SMEM)
    vmem = pl.BlockSpec(memory_space=VMEM)
    hbm = pl.BlockSpec(memory_space=pl.ANY)
    f32, bf16 = jnp.float32, jnp.bfloat16
    in_hbm = [
        pltpu.with_memory_space_constraint(a, pltpu.HBM)
        for a in (tokens, wq, wk, wv, wo, cosine, sine)
    ]
    tokens, wq, wk, wv, wo, cosine, sine = in_hbm
    return pl.pallas_call(
        functools.partial(layer_kernel, mp_size),
        out_shape=[VMEM((slots, share), f32)] * mp_size,
        in_specs=[smem, hbm, hbm, hbm, hbm, hbm, hbm, hbm, hbm, hbm, hbm],
        out_specs=[vmem] * mp_size,
        scratch_shapes=[
            VMEM((buffer_len, width), bf16),
            VMEM(wq.shape, bf16),
            VMEM((width, 2 * HEAD_DIM), bf16),
            VMEM(wo.shape, bf16),
            VMEM((buffer_len, HEAD_DIM), f32),
            VMEM((buffer_len, HEAD_DIM), f32),
            VMEM((ROWS, wq.shape[1]), f32),
            VMEM((ROWS, 2 * HEAD_DIM), f32),
            VMEM((ROWS, HEAD_DIM), f32),
            VMEM((heads, buffer_len, HEAD_DIM), bf16),
            VMEM((buffer_len, HEAD_DIM), bf16),
            VMEM((buffer_len, HEAD_DIM), bf16),
            VMEM((buffer_len, HEAD_DIM), jnp.int32),
            VMEM((16, share), f32),
            VMEM((8, buffer_len), f32),
            VMEM((slots, width), f32),
            VMEM((1, width), bf16),
            VMEM((width,), bf16),
            pltpu.SMEM((slots,), jnp.int32),
            pltpu.SMEM((slots,), jnp.int32),
            pltpu.SemaphoreType.DMA((blocks - 1,)),
            pltpu.SemaphoreType.DMA((CHUNKS, 4)),
            pltpu.SemaphoreType.DMA((6,)),
        ],
        compiler_params=pltpu.CompilerParams(vmem_limit_bytes=LAYER_VMEM),
        name="layer",
    )(rank, starts, lengths, tokens, gain, wq, wk, wv, wo, cosine, sine)


def gram_kernel(dp_size, rank_ref, *rest):
    parts, (all_ref, gram_ref) = rest[:dp_size], rest[dp_size:]
    rank = rank_ref[0]
    rows = parts[0].shape[0]
    for k in range(dp_size):
        owner = lax.rem(rank + dp_size - k, dp_size)
        all_ref[pl.ds(pl.multiple_of(owner * rows, rows), rows), :] = parts[k][...]
    pooled = all_ref[...]
    gram_ref[...] = lax.dot_general(
        pooled, pooled, (((1,), (1,)), ((), ())), precision=HIGHEST,
        preferred_element_type=jnp.float32,
    )


def score_kernel(mp_size, width, episodes, rank_ref, *rest):
    grams = rest[:mp_size]
    all_ref, ids_ref, own_ref, log_ref, proto_ref, cross_s = rest[mp_size:]
    rank = rank_ref[0]
    total = all_ref.shape[0]
    own_count = log_ref.shape[0]
    classes = episodes * WAYS
    gram = grams[0][...]
    for k in range(1, mp_size):
        gram = gram + grams[k][...]
    eye = lax.broadcasted_iota(jnp.int32, (total, total), 0) == lax.broadcasted_iota(
        jnp.int32, (total, total), 1
    )
    square = jnp.sum(jnp.where(eye, gram, 0.0), axis=1, keepdims=True)
    scale = lax.rsqrt(square * (1.0 / width) + 1e-06)
    label = jnp.max(jnp.where(eye, ids_ref[...], -1), axis=1, keepdims=True)
    class_of = lax.broadcasted_iota(jnp.int32, (total, classes), 1)
    select = jnp.where(label == class_of, scale, 0.0)
    cross = jnp.dot(gram, select, precision=HIGHEST, preferred_element_type=jnp.float32)
    norm = jnp.maximum(jnp.sum(cross * select, axis=0, keepdims=True), 0.0)
    proto_scale = lax.rsqrt(norm * (1.0 / width) + 1e-06)
    proto_ref[...] = lax.dot_general(
        select * proto_scale, all_ref[...], (((0,), (0,)), ((), ())), precision=HIGHEST,
        preferred_element_type=jnp.float32,
    )
    cross_s[...] = (
        square * scale * scale
        + norm * proto_scale * proto_scale
        - 2.0 * (scale * proto_scale) * cross
    )
    distance = cross_s[pl.ds(pl.multiple_of(rank * own_count, own_count), own_count), :]
    own_episode = own_ref[:, 0:1]
    own_query = own_ref[:, 1:2]
    picked = distance[:, :WAYS]
    for e in range(1, episodes):
        picked = jnp.where(own_episode == e, distance[:, e * WAYS : (e + 1) * WAYS], picked)
    logits = picked * (-1.0 / math.sqrt(width))
    peak = jnp.max(logits, axis=1, keepdims=True)
    shifted = logits - peak
    out = shifted - jnp.log(jnp.sum(jnp.exp(shifted), axis=1, keepdims=True))
    log_ref[...] = jnp.where(own_query == 1, out, 0.0)


def in_vmem(x):
    return pltpu.with_memory_space_constraint(x, VMEM)


def shifted_by(axis, size, k):
    return [(i, (i + k) % size) for i in range(size)]


def per_device(
    tokens, norm_gain, w_query, w_key, w_value, w_out,
    seq_starts, seq_lengths, episode_ids, class_ids, query_flags,
):
    width = tokens.shape[1]
    slots = seq_starts.shape[0]
    total = episode_ids.shape[0]
    episodes = max(1, total // (2 * WAYS))
    mp_size = lax.axis_size("mp")
    dp_size = lax.axis_size("dp")
    mp_rank = lax.axis_index("mp")
    dp_rank = lax.axis_index("dp")
    share = width // mp_size
    f32 = jnp.float32
    vmem = pl.BlockSpec(memory_space=VMEM)
    smem = pl.BlockSpec(memory_space=pltpu.SMEM)

    parts = layer_call(
        mp_size, mp_rank.reshape(1), seq_starts, seq_lengths, tokens,
        norm_gain, w_query, w_key, w_value, w_out,
    )
    pooled = parts[0]
    arrived = [
        lax.ppermute(parts[k], "mp", shifted_by("mp", mp_size, k)) for k in range(1, mp_size)
    ]
    for a in arrived:
        pooled = pooled + a

    gathered = [pooled] + [
        lax.ppermute(pooled, "dp", shifted_by("dp", dp_size, k)) for k in range(1, dp_size)
    ]
    everyone, gram = pl.pallas_call(
        functools.partial(gram_kernel, dp_size),
        out_shape=[VMEM((total, share), f32), VMEM((total, total), f32)],
        in_specs=[smem] + [vmem] * dp_size,
        out_specs=[vmem, vmem],
        compiler_params=pltpu.CompilerParams(vmem_limit_bytes=SMALL_VMEM),
        name="gram",
    )(dp_rank.reshape(1), *[in_vmem(g) for g in gathered])

    grams = [gram] + [
        lax.ppermute(gram, "mp", shifted_by("mp", mp_size, k)) for k in range(1, mp_size)
    ]
    ids = jnp.where(query_flags == 0, episode_ids * WAYS + class_ids, -1).reshape(1, total)
    own_first = dp_rank * slots
    own = jnp.stack(
        [
            lax.dynamic_slice_in_dim(episode_ids, own_first, slots, 0),
            lax.dynamic_slice_in_dim(query_flags, own_first, slots, 0),
        ],
        axis=1,
    )
    log_probs, prototypes = pl.pallas_call(
        functools.partial(score_kernel, mp_size, width, episodes),
        out_shape=[
            jax.ShapeDtypeStruct((slots, WAYS), f32),
            jax.ShapeDtypeStruct((episodes * WAYS, share), f32),
        ],
        in_specs=[smem] + [vmem] * (mp_size + 3),
        out_specs=[vmem, vmem],
        scratch_shapes=[VMEM((total, episodes * WAYS), f32)],
        compiler_params=pltpu.CompilerParams(vmem_limit_bytes=SMALL_VMEM),
        name="score",
    )(dp_rank.reshape(1), *[in_vmem(g) for g in grams], in_vmem(everyone), ids, own)
    return log_probs, prototypes


def solution(mesh):
    placed = (
        P("dp", None), P(), P(None, "mp"), P(None, "mp"), P(None, "mp"), P("mp", None),
        P("dp"), P("dp"), P(), P(), P(),
    )
    return jax.shard_map(
        per_device,
        mesh=mesh,
        in_specs=placed,
        out_specs=(P("dp", None), P(None, "mp")),
        check_vma=False,
    )
```

```python
import functools
import math

import jax
import jax.numpy as jnp
import numpy as np
from jax import lax
from jax.experimental import pallas as pl
from jax.experimental.pallas import tpu as pltpu
from jax.sharding import PartitionSpec as P

HEAD_DIM = 128
WAYS = 32
MAX_LEN = 640
ROPE_BASE = 500000.0
NEG_FILL = -1e30
ROWS = 768
QBLOCK = 128
AROWS = 256
CHUNKS = 2
LAYER_VMEM = 56 * 1024 * 1024
SMALL_VMEM = 8 * 1024 * 1024

HIGHEST = lax.Precision.HIGHEST
VMEM = pltpu.VMEM


def rope_tables(rows):
    half = HEAD_DIM // 2
    freq = ROPE_BASE ** (-(np.arange(half) * 2.0 / HEAD_DIM))
    angle = np.arange(rows)[:, None] * freq[None, :]
    cosine = np.concatenate([np.cos(angle), np.cos(angle)], axis=1)
    sine = np.concatenate([-np.sin(angle), np.sin(angle)], axis=1)
    return cosine.astype(np.float32), sine.astype(np.float32)


def layer_kernel(
    mp_size,
    rank_ref,
    starts_hbm,
    lengths_hbm,
    tokens_hbm,
    gain_hbm,
    wq_hbm,
    wk_hbm,
    wv_hbm,
    wo_hbm,
    cos_hbm,
    sin_hbm,
    *rest,
):
    outs = rest[:mp_size]
    (
        x_s, wq_s, wkv_s, wo_s, cos_s, sin_s, raw_q, raw_kv, square_s,
        q_s, k_s, v_s, first_s, tok_s, wacc_s, hp_s, gain_s,
        gain_flat, starts_ref, lengths_ref, xsem, wsem, tsem,
    ) = rest[mp_size:]
    buffer_len, width = x_s.shape
    q_cols = wq_hbm.shape[1]
    heads = q_cols // HEAD_DIM
    blocks = buffer_len // ROWS
    slots = starts_hbm.shape[0]
    share = width // mp_size
    depth = width // CHUNKS
    rank = rank_ref[0]

    def x_copy(i):
        rows = pl.ds(i * ROWS, ROWS)
        return pltpu.make_async_copy(tokens_hbm.at[rows], x_s.at[rows], xsem.at[i - 1])

    def chunk_copies(c):
        part = pl.ds(pl.multiple_of(c * depth, depth), depth)
        rows = pl.ds(0, ROWS)
        return [
            pltpu.make_async_copy(
                tokens_hbm.at[rows, part], x_s.at[rows, part], wsem.at[c, 0]
            ),
            pltpu.make_async_copy(wq_hbm.at[part], wq_s.at[part], wsem.at[c, 1]),
            pltpu.make_async_copy(
                wk_hbm.at[part], wkv_s.at[part, pl.ds(0, HEAD_DIM)], wsem.at[c, 2]
            ),
            pltpu.make_async_copy(
                wv_hbm.at[part], wkv_s.at[part, pl.ds(HEAD_DIM, HEAD_DIM)], wsem.at[c, 3]
            ),
        ]

    table_copies = [
        pltpu.make_async_copy(cos_hbm, cos_s, tsem.at[0]),
        pltpu.make_async_copy(sin_hbm, sin_s, tsem.at[1]),
    ]
    out_copy = pltpu.make_async_copy(wo_hbm, wo_s, tsem.at[2])
    small_copies = [
        pltpu.make_async_copy(starts_hbm, starts_ref, tsem.at[3]),
        pltpu.make_async_copy(lengths_hbm, lengths_ref, tsem.at[4]),
        pltpu.make_async_copy(gain_hbm, gain_flat, tsem.at[5]),
    ]
    for copy in small_copies:
        copy.start()
    for c in range(CHUNKS):
        for copy in chunk_copies(c):
            copy.start()
    x_copy(1).start()
    for copy in table_copies:
        copy.start()
    for i in range(2, blocks):
        x_copy(i).start()
    out_copy.start()

    for copy in small_copies:
        copy.wait()

    row = lax.broadcasted_iota(jnp.int32, (1, buffer_len), 1)
    first = row
    for s in range(slots):
        begin = starts_ref[s]
        inside = (row >= begin) & (row < begin + lengths_ref[s])
        first = jnp.where(inside, begin, first)
    first_s[...] = first
    gain_s[...] = gain_flat[...].reshape(1, width)
    tok_s[...] = jnp.zeros_like(tok_s)
    wacc_s[...] = jnp.zeros_like(wacc_s)
    raw_q[...] = jnp.zeros_like(raw_q)
    raw_kv[...] = jnp.zeros_like(raw_kv)
    square_s[...] = jnp.zeros_like(square_s)

    def members(row_first, count, sublanes):
        row = row_first + lax.broadcasted_iota(jnp.int32, (sublanes, count), 1)
        slot = lax.broadcasted_iota(jnp.int32, (sublanes, count), 0)
        low = jnp.zeros((sublanes, count), jnp.int32)
        high = jnp.zeros((sublanes, count), jnp.int32)
        for s in range(slots):
            low = jnp.where(slot == s, starts_ref[s], low)
            high = jnp.where(slot == s, starts_ref[s] + lengths_ref[s], high)
        return jnp.where((row >= low) & (row < high), 1.0, 0.0)

    share_cols = pl.ds(pl.multiple_of(rank * share, share), share)
    score_scale = math.log2(math.e) / math.sqrt(HEAD_DIM)
    half = ROWS // 2

    def dots(scaled, w_q, w_kv):
        f32 = jnp.float32
        return (
            jnp.dot(scaled, w_q, preferred_element_type=f32),
            jnp.dot(scaled[:half], w_kv, preferred_element_type=f32),
            jnp.dot(scaled[half:], w_kv, preferred_element_type=f32),
        )

    def lane_squares(x):
        wide = x.astype(jnp.float32)
        total = None
        for c in range(x.shape[1] // HEAD_DIM):
            piece = wide[:, c * HEAD_DIM : (c + 1) * HEAD_DIM]
            total = piece * piece if total is None else total + piece * piece
        return total

    def token_sums(i, rows):
        member = members(i * ROWS, ROWS, 16).astype(jnp.bfloat16)
        tok_s[...] += jnp.dot(
            member, x_s[rows, share_cols], preferred_element_type=jnp.float32
        )

    def first_chunk(c, _):
        for copy in chunk_copies(c):
            copy.wait()
        part = pl.ds(pl.multiple_of(c * depth, depth), depth)
        x = x_s[0:ROWS, part]
        q, kv_a, kv_b = dots(x * gain_s[:, part], wq_s[part, :], wkv_s[part, :])
        raw_q[...] += q
        raw_kv[0:half, :] += kv_a
        raw_kv[half:, :] += kv_b
        square_s[...] += lane_squares(x)
        return 0

    def project(i):
        rows = pl.ds(pl.multiple_of(i * ROWS, ROWS), ROWS)
        x = x_s[rows, :]
        q, kv_a, kv_b = dots(x * gain_s[...], wq_s[...], wkv_s[...])
        raw_q[...] = q
        raw_kv[0:half, :] = kv_a
        raw_kv[half:, :] = kv_b
        square_s[...] = lane_squares(x)
        token_sums(i, rows)

    def finish(i):
        rows = pl.ds(pl.multiple_of(i * ROWS, ROWS), ROWS)
        square = jnp.sum(square_s[...], axis=1, keepdims=True)
        inv = lax.rsqrt(square * (1.0 / width) + 1e-05)
        cosine = cos_s[rows, :] * inv
        sine = sin_s[rows, :] * inv
        q_cosine = cosine * score_scale
        q_sine = sine * score_scale
        for h in range(heads):
            head = raw_q[:, h * HEAD_DIM : (h + 1) * HEAD_DIM]
            turned = head * q_cosine + pltpu.roll(head, HEAD_DIM // 2, 1) * q_sine
            turned = turned.astype(jnp.bfloat16)
            for b in range(ROWS // QBLOCK):
                q_s[i * (ROWS // QBLOCK) + b, h * QBLOCK : (h + 1) * QBLOCK, :] = turned[
                    b * QBLOCK : (b + 1) * QBLOCK
                ]
        key = raw_kv[:, :HEAD_DIM]
        turned = key * cosine + pltpu.roll(key, HEAD_DIM // 2, 1) * sine
        k_s[rows, :] = turned.astype(jnp.bfloat16)
        v_s[rows, :] = (raw_kv[:, HEAD_DIM:] * inv).astype(jnp.bfloat16)

    lax.fori_loop(0, CHUNKS, first_chunk, 0)
    token_sums(0, pl.ds(0, ROWS))
    for copy in table_copies:
        copy.wait()

    def step(i, _):
        x_copy(i).wait()
        finish(i - 1)
        project(i)
        return 0

    for i in range(1, blocks):
        step(i, 0)
    finish(blocks - 1)

    most = (MAX_LEN - 1 + QBLOCK - 1) // QBLOCK
    parts_per = AROWS // QBLOCK

    def attend(i, _):
        top = i * AROWS
        lowest = top
        for s in range(slots):
            begin = starts_ref[s]
            inside = (top >= begin) & (top < begin + lengths_ref[s])
            lowest = jnp.where(inside, begin, lowest)
        ahead = i * parts_per - lowest // QBLOCK
        for n in range(most + 1):

            @pl.when(ahead == n)
            def _(n=n):
                spans, scores, tables = [], [], []
                for part in range(parts_per):
                    before = min(n + part, most)
                    keys = (before + 1) * QBLOCK
                    row_first = pl.multiple_of(top + part * QBLOCK, QBLOCK)
                    key_first = pl.multiple_of(row_first - before * QBLOCK, QBLOCK)
                    spans.append((keys, row_first, key_first))
                    scores.append(
                        lax.dot_general(
                            k_s[pl.ds(key_first, keys), :],
                            q_s[i * parts_per + part],
                            (((1,), (1,)), ((), ())),
                            preferred_element_type=jnp.float32,
                        )
                    )
                for part in range(parts_per):
                    keys, row_first, key_first = spans[part]
                    first = first_s[:, pl.ds(row_first, QBLOCK)]
                    row = row_first + lax.broadcasted_iota(jnp.int32, (keys, QBLOCK), 1)
                    key = key_first + lax.broadcasted_iota(jnp.int32, (keys, QBLOCK), 0)
                    permitted = (key >= first) & (key <= row)
                    powers, weights = [], []
                    for h in range(heads):
                        score = scores[part][:, h * QBLOCK : (h + 1) * QBLOCK]
                        score = jnp.where(permitted, score, NEG_FILL)
                        peak = jnp.max(score, axis=0, keepdims=True)
                        power = jnp.exp2(score - peak)
                        weight = 1.0 / jnp.sum(power, axis=0, keepdims=True)
                        powers.append(power.astype(jnp.bfloat16))
                        high = weight.astype(jnp.bfloat16).astype(jnp.float32)
                        place = lax.broadcasted_iota(jnp.int32, (16, QBLOCK), 0)
                        weights.append(
                            jnp.where(
                                place == h, high, jnp.where(place == h + 8, weight - high, 0.0)
                            ).astype(jnp.bfloat16)
                        )
                    tables.append(
                        (jnp.concatenate(weights, axis=1), jnp.concatenate(powers, axis=1))
                    )
                columns = [
                    lax.dot_general(
                        weight, power, (((1,), (1,)), ((), ())),
                        preferred_element_type=jnp.float32,
                    )
                    for weight, power in tables
                ]
                for part in range(parts_per):
                    keys, _, key_first = spans[part]
                    wacc_s[:, pl.ds(key_first, keys)] += columns[part]

        return 0

    lax.fori_loop(0, buffer_len // AROWS, attend, 0)

    member = members(0, buffer_len, 8)
    column_sums = wacc_s[0:8, :] + wacc_s[8:16, :]
    weighted = jnp.concatenate(
        [member * column_sums[h : h + 1, :] for h in range(heads)], axis=0
    )
    count = heads * 8
    high = weighted.astype(jnp.bfloat16)
    low = (weighted - high.astype(jnp.float32)).astype(jnp.bfloat16)
    both = jnp.dot(
        jnp.concatenate([high, low], axis=0), v_s[...], preferred_element_type=jnp.float32
    )
    sums = both[:count] + both[count:]
    sums = jnp.concatenate([sums[h * 8 : (h + 1) * 8] for h in range(heads)], axis=1)
    high = sums.astype(jnp.bfloat16)
    low = (sums - high.astype(jnp.float32)).astype(jnp.bfloat16)
    out_copy.wait()
    parts = jnp.dot(
        jnp.concatenate([high, low], axis=0), wo_s[...], preferred_element_type=jnp.float32
    )
    slot = lax.broadcasted_iota(jnp.int32, (8, HEAD_DIM), 0)
    tokens_in = jnp.ones((8, HEAD_DIM), jnp.int32)
    for s in range(slots):
        tokens_in = jnp.where(slot == s, lengths_ref[s], tokens_in)
    per_token = (1.0 / tokens_in.astype(jnp.float32))[:, 0:1]
    hp_s[...] = (parts[:8] + parts[8:]) * per_token
    outs[0][...] = hp_s[:, share_cols] + tok_s[0:8, :] * per_token
    for k in range(1, mp_size):
        other = rank ^ k
        outs[k][...] = hp_s[:, pl.ds(pl.multiple_of(other * share, share), share)]


def layer_call(mp_size, rank, starts, lengths, tokens, gain, wq, wk, wv, wo):
    buffer_len, width = tokens.shape
    slots = starts.shape[0]
    assert slots == 8 and wk.shape[1] == HEAD_DIM
    heads = wq.shape[1] // HEAD_DIM
    blocks = buffer_len // ROWS
    share = width // mp_size
    cosine, sine = rope_tables(buffer_len)
    smem = pl.BlockSpec(memory_space=pltpu.SMEM)
    vmem = pl.BlockSpec(memory_space=VMEM)
    hbm = pl.BlockSpec(memory_space=pl.ANY)
    f32, bf16 = jnp.float32, jnp.bfloat16
    in_hbm = [
        pltpu.with_memory_space_constraint(a, pltpu.HBM)
        for a in (tokens, wq, wk, wv, wo, cosine, sine)
    ]
    tokens, wq, wk, wv, wo, cosine, sine = in_hbm
    return pl.pallas_call(
        functools.partial(layer_kernel, mp_size),
        out_shape=[VMEM((slots, share), f32)] * mp_size,
        in_specs=[smem, hbm, hbm, hbm, hbm, hbm, hbm, hbm, hbm, hbm, hbm],
        out_specs=[vmem] * mp_size,
        scratch_shapes=[
            VMEM((buffer_len, width), bf16),
            VMEM(wq.shape, bf16),
            VMEM((width, 2 * HEAD_DIM), bf16),
            VMEM(wo.shape, bf16),
            VMEM((buffer_len, HEAD_DIM), f32),
            VMEM((buffer_len, HEAD_DIM), f32),
            VMEM((ROWS, wq.shape[1]), f32),
            VMEM((ROWS, 2 * HEAD_DIM), f32),
            VMEM((ROWS, HEAD_DIM), f32),
            VMEM((buffer_len // QBLOCK, heads * QBLOCK, HEAD_DIM), bf16),
            VMEM((buffer_len, HEAD_DIM), bf16),
            VMEM((buffer_len, HEAD_DIM), bf16),
            VMEM((1, buffer_len), jnp.int32),
            VMEM((16, share), f32),
            VMEM((16, buffer_len), f32),
            VMEM((slots, width), f32),
            VMEM((1, width), bf16),
            VMEM((width,), bf16),
            pltpu.SMEM((slots,), jnp.int32),
            pltpu.SMEM((slots,), jnp.int32),
            pltpu.SemaphoreType.DMA((blocks - 1,)),
            pltpu.SemaphoreType.DMA((CHUNKS, 4)),
            pltpu.SemaphoreType.DMA((6,)),
        ],
        compiler_params=pltpu.CompilerParams(vmem_limit_bytes=LAYER_VMEM),
        name="layer",
    )(rank, starts, lengths, tokens, gain, wq, wk, wv, wo, cosine, sine)


def gram_kernel(dp_size, rank_ref, *rest):
    parts, (all_ref, gram_ref) = rest[: dp_size // 2], rest[dp_size // 2 :]
    rank = rank_ref[0]
    rows = parts[0].shape[0] // 2
    for j in range(dp_size // 2):
        for side in range(2):
            owner = rank ^ (2 * j + side)
            all_ref[pl.ds(pl.multiple_of(owner * rows, rows), rows), :] = parts[j][
                side * rows : (side + 1) * rows, :
            ]
    pooled = all_ref[...]
    gram_ref[...] = lax.dot_general(
        pooled, pooled, (((1,), (1,)), ((), ())), precision=HIGHEST,
        preferred_element_type=jnp.float32,
    )


def score_kernel(mp_size, width, episodes, rank_ref, *rest):
    grams = rest[:mp_size]
    all_ref, ids_ref, own_ref, log_ref, proto_ref, cross_s = rest[mp_size:]
    rank = rank_ref[0]
    total = all_ref.shape[0]
    own_count = log_ref.shape[0]
    classes = episodes * WAYS
    gram = grams[0][...]
    for k in range(1, mp_size):
        gram = gram + grams[k][...]
    eye = lax.broadcasted_iota(jnp.int32, (total, total), 0) == lax.broadcasted_iota(
        jnp.int32, (total, total), 1
    )
    square = jnp.sum(jnp.where(eye, gram, 0.0), axis=1, keepdims=True)
    scale = lax.rsqrt(square * (1.0 / width) + 1e-06)
    label = jnp.max(jnp.where(eye, ids_ref[...], -1), axis=1, keepdims=True)
    class_of = lax.broadcasted_iota(jnp.int32, (total, classes), 1)
    select = jnp.where(label == class_of, scale, 0.0)
    cross = jnp.dot(gram, select, precision=HIGHEST, preferred_element_type=jnp.float32)
    norm = jnp.maximum(jnp.sum(cross * select, axis=0, keepdims=True), 0.0)
    proto_scale = lax.rsqrt(norm * (1.0 / width) + 1e-06)
    proto_ref[...] = lax.dot_general(
        select * proto_scale, all_ref[...], (((0,), (0,)), ((), ())), precision=HIGHEST,
        preferred_element_type=jnp.float32,
    )
    cross_s[...] = (
        square * scale * scale
        + norm * proto_scale * proto_scale
        - 2.0 * (scale * proto_scale) * cross
    )
    distance = cross_s[pl.ds(pl.multiple_of(rank * own_count, own_count), own_count), :]
    own_episode = own_ref[:, 0:1]
    own_query = own_ref[:, 1:2]
    picked = distance[:, :WAYS]
    for e in range(1, episodes):
        picked = jnp.where(own_episode == e, distance[:, e * WAYS : (e + 1) * WAYS], picked)
    logits = picked * (-1.0 / math.sqrt(width))
    peak = jnp.max(logits, axis=1, keepdims=True)
    shifted = logits - peak
    out = shifted - jnp.log(jnp.sum(jnp.exp(shifted), axis=1, keepdims=True))
    log_ref[...] = jnp.where(own_query == 1, out, 0.0)


def in_vmem(x):
    return pltpu.with_memory_space_constraint(x, VMEM)


def paired(size, k):
    return [(i, i ^ k) for i in range(size)]


def MP_ORDER(size):
    return range(size - 1, 0, -1)


def DP_ORDER(size):
    return range(size - 2, 0, -2)


def per_device(
    tokens, norm_gain, w_query, w_key, w_value, w_out,
    seq_starts, seq_lengths, episode_ids, class_ids, query_flags,
):
    width = tokens.shape[1]
    slots = seq_starts.shape[0]
    total = episode_ids.shape[0]
    episodes = max(1, total // (2 * WAYS))
    mp_size = lax.axis_size("mp")
    dp_size = lax.axis_size("dp")
    mp_rank = lax.axis_index("mp")
    dp_rank = lax.axis_index("dp")
    share = width // mp_size
    f32 = jnp.float32
    vmem = pl.BlockSpec(memory_space=VMEM)
    smem = pl.BlockSpec(memory_space=pltpu.SMEM)

    parts = layer_call(
        mp_size, mp_rank.reshape(1), seq_starts, seq_lengths, tokens,
        norm_gain, w_query, w_key, w_value, w_out,
    )
    pooled = parts[0]
    for k in MP_ORDER(mp_size):
        pooled = pooled + lax.ppermute(parts[k], "mp", paired(mp_size, k))

    partner = lax.ppermute(pooled, "dp", paired(dp_size, 1))
    pair = jnp.concatenate([pooled, partner], axis=0)
    gathered = {0: pair}
    for k in DP_ORDER(dp_size):
        gathered[k] = lax.ppermute(pair, "dp", paired(dp_size, k))
    everyone, gram = pl.pallas_call(
        functools.partial(gram_kernel, dp_size),
        out_shape=[VMEM((total, share), f32), VMEM((total, total), f32)],
        in_specs=[smem] + [vmem] * (dp_size // 2),
        out_specs=[vmem, vmem],
        compiler_params=pltpu.CompilerParams(vmem_limit_bytes=SMALL_VMEM),
        name="gram",
    )(dp_rank.reshape(1), *[in_vmem(gathered[k]) for k in range(0, dp_size, 2)])

    grams = [gram] + [lax.ppermute(gram, "mp", paired(mp_size, k)) for k in MP_ORDER(mp_size)]
    ids = jnp.where(query_flags == 0, episode_ids * WAYS + class_ids, -1).reshape(1, total)
    own_first = dp_rank * slots
    own = jnp.stack(
        [
            lax.dynamic_slice_in_dim(episode_ids, own_first, slots, 0),
            lax.dynamic_slice_in_dim(query_flags, own_first, slots, 0),
        ],
        axis=1,
    )
    log_probs, prototypes = pl.pallas_call(
        functools.partial(score_kernel, mp_size, width, episodes),
        out_shape=[
            jax.ShapeDtypeStruct((slots, WAYS), f32),
            jax.ShapeDtypeStruct((episodes * WAYS, share), f32),
        ],
        in_specs=[smem] + [vmem] * (mp_size + 3),
        out_specs=[vmem, vmem],
        scratch_shapes=[VMEM((total, episodes * WAYS), f32)],
        compiler_params=pltpu.CompilerParams(vmem_limit_bytes=SMALL_VMEM),
        name="score",
    )(dp_rank.reshape(1), *[in_vmem(g) for g in grams], in_vmem(everyone), ids, own)
    return log_probs, prototypes


def solution(mesh):
    placed = (
        P("dp", None), P(), P(None, "mp"), P(None, "mp"), P(None, "mp"), P("mp", None),
        P("dp"), P("dp"), P(), P(), P(),
    )
    return jax.shard_map(
        per_device,
        mesh=mesh,
        in_specs=placed,
        out_specs=(P("dp", None), P(None, "mp")),
        check_vma=False,
    )
```

```python
import functools
import math

import jax
import jax.numpy as jnp
import numpy as np
from jax import lax
from jax.experimental import pallas as pl
from jax.experimental.pallas import tpu as pltpu
from jax.sharding import PartitionSpec as P

HEAD_DIM = 128
WAYS = 32
MAX_LEN = 640
ROPE_BASE = 500000.0
NEG_FILL = -1e30
ROWS = 768
QBLOCK = 128
AROWS = 256
CHUNKS = 2
STATIC_GROUP = 1
LAYER_VMEM = 56 * 1024 * 1024
SMALL_VMEM = 8 * 1024 * 1024

HIGHEST = lax.Precision.HIGHEST
VMEM = pltpu.VMEM


def rope_tables(rows):
    half = HEAD_DIM // 2
    freq = ROPE_BASE ** (-(np.arange(half) * 2.0 / HEAD_DIM))
    angle = np.arange(rows)[:, None] * freq[None, :]
    cosine = np.concatenate([np.cos(angle), np.cos(angle)], axis=1)
    sine = np.concatenate([-np.sin(angle), np.sin(angle)], axis=1)
    return cosine.astype(np.float32), sine.astype(np.float32)


def layer_kernel(
    mp_size,
    rank_ref,
    starts_hbm,
    lengths_hbm,
    tokens_hbm,
    gain_hbm,
    wq_hbm,
    wk_hbm,
    wv_hbm,
    wo_hbm,
    cos_hbm,
    sin_hbm,
    *rest,
):
    outs = rest[:mp_size]
    (
        x_s, wq_s, wkv_s, wo_s, cos_s, sin_s, raw_q, raw_kv, square_s,
        q_s, k_s, v_s, first_s, tok_s, wacc_s, hp_s, gain_s,
        gain_flat, starts_ref, lengths_ref, xsem, wsem, tsem,
    ) = rest[mp_size:]
    buffer_len, width = x_s.shape
    q_cols = wq_hbm.shape[1]
    heads = q_cols // HEAD_DIM
    blocks = buffer_len // ROWS
    slots = starts_hbm.shape[0]
    share = width // mp_size
    depth = width // CHUNKS
    rank = rank_ref[0]

    def x_copy(i):
        rows = pl.ds(i * ROWS, ROWS)
        return pltpu.make_async_copy(tokens_hbm.at[rows], x_s.at[rows], xsem.at[i - 1])

    def chunk_copies(c):
        part = pl.ds(pl.multiple_of(c * depth, depth), depth)
        rows = pl.ds(0, ROWS)
        return [
            pltpu.make_async_copy(
                tokens_hbm.at[rows, part], x_s.at[rows, part], wsem.at[c, 0]
            ),
            pltpu.make_async_copy(wq_hbm.at[part], wq_s.at[part], wsem.at[c, 1]),
            pltpu.make_async_copy(
                wk_hbm.at[part], wkv_s.at[part, pl.ds(0, HEAD_DIM)], wsem.at[c, 2]
            ),
            pltpu.make_async_copy(
                wv_hbm.at[part], wkv_s.at[part, pl.ds(HEAD_DIM, HEAD_DIM)], wsem.at[c, 3]
            ),
        ]

    table_copies = [
        pltpu.make_async_copy(cos_hbm, cos_s, tsem.at[0]),
        pltpu.make_async_copy(sin_hbm, sin_s, tsem.at[1]),
    ]
    out_copy = pltpu.make_async_copy(wo_hbm, wo_s, tsem.at[2])
    small_copies = [
        pltpu.make_async_copy(starts_hbm, starts_ref, tsem.at[3]),
        pltpu.make_async_copy(lengths_hbm, lengths_ref, tsem.at[4]),
        pltpu.make_async_copy(gain_hbm, gain_flat, tsem.at[5]),
    ]
    for copy in small_copies:
        copy.start()
    for c in range(CHUNKS):
        for copy in chunk_copies(c):
            copy.start()
    x_copy(1).start()
    for copy in table_copies:
        copy.start()
    for i in range(2, blocks):
        x_copy(i).start()
    out_copy.start()

    for copy in small_copies:
        copy.wait()

    row = lax.broadcasted_iota(jnp.int32, (1, buffer_len), 1)
    first = row
    for s in range(slots):
        begin = starts_ref[s]
        inside = (row >= begin) & (row < begin + lengths_ref[s])
        first = jnp.where(inside, begin, first)
    first_s[...] = first
    gain_s[...] = gain_flat[...].reshape(1, width)
    tok_s[...] = jnp.zeros_like(tok_s)
    wacc_s[...] = jnp.zeros_like(wacc_s)
    raw_q[...] = jnp.zeros_like(raw_q)
    raw_kv[...] = jnp.zeros_like(raw_kv)
    square_s[...] = jnp.zeros_like(square_s)

    def members(row_first, count, sublanes):
        row = row_first + lax.broadcasted_iota(jnp.int32, (sublanes, count), 1)
        slot = lax.broadcasted_iota(jnp.int32, (sublanes, count), 0)
        low = jnp.zeros((sublanes, count), jnp.int32)
        high = jnp.zeros((sublanes, count), jnp.int32)
        for s in range(slots):
            low = jnp.where(slot == s, starts_ref[s], low)
            high = jnp.where(slot == s, starts_ref[s] + lengths_ref[s], high)
        return jnp.where((row >= low) & (row < high), 1.0, 0.0)

    share_cols = pl.ds(pl.multiple_of(rank * share, share), share)
    score_scale = math.log2(math.e) / math.sqrt(HEAD_DIM)
    half = ROWS // 2

    def dots(scaled, w_q, w_kv):
        f32 = jnp.float32
        return (
            jnp.dot(scaled, w_q, preferred_element_type=f32),
            jnp.dot(scaled[:half], w_kv, preferred_element_type=f32),
            jnp.dot(scaled[half:], w_kv, preferred_element_type=f32),
        )

    def lane_squares(x):
        wide = x.astype(jnp.float32)
        total = None
        for c in range(x.shape[1] // HEAD_DIM):
            piece = wide[:, c * HEAD_DIM : (c + 1) * HEAD_DIM]
            total = piece * piece if total is None else total + piece * piece
        return total

    def token_sums(i, rows):
        member = members(i * ROWS, ROWS, 16).astype(jnp.bfloat16)
        tok_s[...] += jnp.dot(
            member, x_s[rows, share_cols], preferred_element_type=jnp.float32
        )

    def first_chunk(c, _):
        for copy in chunk_copies(c):
            copy.wait()
        part = pl.ds(pl.multiple_of(c * depth, depth), depth)
        x = x_s[0:ROWS, part]
        q, kv_a, kv_b = dots(x * gain_s[:, part], wq_s[part, :], wkv_s[part, :])
        raw_q[...] += q
        raw_kv[0:half, :] += kv_a
        raw_kv[half:, :] += kv_b
        square_s[...] += lane_squares(x)
        return 0

    def project(i, first, count):
        rows = pl.ds(pl.multiple_of(i * ROWS + first, QBLOCK), count)
        x = x_s[rows, :]
        scaled = x * gain_s[...]
        f32 = jnp.float32
        middle = count // 2
        raw_q[first : first + count, :] = jnp.dot(
            scaled, wq_s[...], preferred_element_type=f32
        )
        for part in range(2):
            span = slice(part * middle, (part + 1) * middle)
            raw_kv[first + part * middle : first + (part + 1) * middle, :] = jnp.dot(
                scaled[span], wkv_s[...], preferred_element_type=f32
            )
        square_s[first : first + count, :] = lane_squares(x)

    def finish(i):
        rows = pl.ds(pl.multiple_of(i * ROWS, ROWS), ROWS)
        square = jnp.sum(square_s[...], axis=1, keepdims=True)
        inv = lax.rsqrt(square * (1.0 / width) + 1e-05)
        cosine = cos_s[rows, :] * inv
        sine = sin_s[rows, :] * inv
        q_cosine = cosine * score_scale
        q_sine = sine * score_scale
        for h in range(heads):
            head = raw_q[:, h * HEAD_DIM : (h + 1) * HEAD_DIM]
            turned = head * q_cosine + pltpu.roll(head, HEAD_DIM // 2, 1) * q_sine
            turned = turned.astype(jnp.bfloat16)
            for b in range(ROWS // QBLOCK):
                q_s[i * (ROWS // QBLOCK) + b, h * QBLOCK : (h + 1) * QBLOCK, :] = turned[
                    b * QBLOCK : (b + 1) * QBLOCK
                ]
        key = raw_kv[:, :HEAD_DIM]
        turned = key * cosine + pltpu.roll(key, HEAD_DIM // 2, 1) * sine
        k_s[rows, :] = turned.astype(jnp.bfloat16)
        v_s[rows, :] = (raw_kv[:, HEAD_DIM:] * inv).astype(jnp.bfloat16)

    lax.fori_loop(0, CHUNKS, first_chunk, 0)
    token_sums(0, pl.ds(0, ROWS))
    for copy in table_copies:
        copy.wait()

    most = (MAX_LEN - 1 + QBLOCK - 1) // QBLOCK
    parts_per = AROWS // QBLOCK

    def attend_windows(windows):
        spans, scores, tables = [], [], []
        for part, before in windows:
            keys = (before + 1) * QBLOCK
            row_first = part * QBLOCK
            key_first = row_first - before * QBLOCK
            if not isinstance(part, int):
                row_first = pl.multiple_of(row_first, QBLOCK)
                key_first = pl.multiple_of(key_first, QBLOCK)
            spans.append((keys, row_first, key_first))
            scores.append(
                lax.dot_general(
                    k_s[pl.ds(key_first, keys), :],
                    q_s[part],
                    (((1,), (1,)), ((), ())),
                    preferred_element_type=jnp.float32,
                )
            )
        for place, (keys, row_first, key_first) in enumerate(spans):
            first = first_s[:, pl.ds(row_first, QBLOCK)]
            row = row_first + lax.broadcasted_iota(jnp.int32, (keys, QBLOCK), 1)
            key = key_first + lax.broadcasted_iota(jnp.int32, (keys, QBLOCK), 0)
            permitted = (key >= first) & (key <= row)
            powers, weights = [], []
            for h in range(heads):
                score = scores[place][:, h * QBLOCK : (h + 1) * QBLOCK]
                score = jnp.where(permitted, score, NEG_FILL)
                peak = jnp.max(score, axis=0, keepdims=True)
                power = jnp.exp2(score - peak)
                weight = 1.0 / jnp.sum(power, axis=0, keepdims=True)
                powers.append(power.astype(jnp.bfloat16))
                high = weight.astype(jnp.bfloat16).astype(jnp.float32)
                slot = lax.broadcasted_iota(jnp.int32, (16, QBLOCK), 0)
                weights.append(
                    jnp.where(
                        slot == h, high, jnp.where(slot == h + 8, weight - high, 0.0)
                    ).astype(jnp.bfloat16)
                )
            tables.append(
                (jnp.concatenate(weights, axis=1), jnp.concatenate(powers, axis=1))
            )
        columns = [
            lax.dot_general(
                weight, power, (((1,), (1,)), ((), ())),
                preferred_element_type=jnp.float32,
            )
            for weight, power in tables
        ]
        for (keys, _, key_first), column in zip(spans, columns):
            wacc_s[:, pl.ds(key_first, keys)] += column

    def step(i, _):
        x_copy(i).wait()
        finish(i - 1)
        per = ROWS // QBLOCK
        pieces = 2
        size = ROWS // pieces
        for piece in range(pieces):
            windows = [
                ((i - 1) * per + p, min((i - 1) * per + p, most))
                for p in range(piece * per // pieces, (piece + 1) * per // pieces)
            ]
            project(i, piece * size, size)
            attend_windows(windows)
        token_sums(i, pl.ds(i * ROWS, ROWS))
        return 0

    for i in range(1, blocks):
        step(i, 0)
    finish(blocks - 1)

    def attend(i, _):
        top = i * AROWS
        lowest = top
        for s in range(slots):
            begin = starts_ref[s]
            inside = (top >= begin) & (top < begin + lengths_ref[s])
            lowest = jnp.where(inside, begin, lowest)
        ahead = i * parts_per - lowest // QBLOCK
        for n in range(most + 1):

            @pl.when(ahead == n)
            def _(n=n):
                attend_windows(
                    [(i * parts_per + p, min(n + p, most)) for p in range(parts_per)]
                )

        return 0

    lax.fori_loop((blocks - 1) * ROWS // AROWS, buffer_len // AROWS, attend, 0)

    member = members(0, buffer_len, 8)
    column_sums = wacc_s[0:8, :] + wacc_s[8:16, :]
    weighted = jnp.concatenate(
        [member * column_sums[h : h + 1, :] for h in range(heads)], axis=0
    )
    count = heads * 8
    high = weighted.astype(jnp.bfloat16)
    low = (weighted - high.astype(jnp.float32)).astype(jnp.bfloat16)
    both = jnp.dot(
        jnp.concatenate([high, low], axis=0), v_s[...], preferred_element_type=jnp.float32
    )
    sums = both[:count] + both[count:]
    sums = jnp.concatenate([sums[h * 8 : (h + 1) * 8] for h in range(heads)], axis=1)
    high = sums.astype(jnp.bfloat16)
    low = (sums - high.astype(jnp.float32)).astype(jnp.bfloat16)
    out_copy.wait()
    parts = jnp.dot(
        jnp.concatenate([high, low], axis=0), wo_s[...], preferred_element_type=jnp.float32
    )
    slot = lax.broadcasted_iota(jnp.int32, (8, HEAD_DIM), 0)
    tokens_in = jnp.ones((8, HEAD_DIM), jnp.int32)
    for s in range(slots):
        tokens_in = jnp.where(slot == s, lengths_ref[s], tokens_in)
    per_token = (1.0 / tokens_in.astype(jnp.float32))[:, 0:1]
    hp_s[...] = (parts[:8] + parts[8:]) * per_token
    outs[0][...] = hp_s[:, share_cols] + tok_s[0:8, :] * per_token
    for k in range(1, mp_size):
        other = rank ^ k
        outs[k][...] = hp_s[:, pl.ds(pl.multiple_of(other * share, share), share)]


def layer_call(mp_size, rank, starts, lengths, tokens, gain, wq, wk, wv, wo):
    buffer_len, width = tokens.shape
    slots = starts.shape[0]
    assert slots == 8 and wk.shape[1] == HEAD_DIM
    heads = wq.shape[1] // HEAD_DIM
    blocks = buffer_len // ROWS
    share = width // mp_size
    cosine, sine = rope_tables(buffer_len)
    smem = pl.BlockSpec(memory_space=pltpu.SMEM)
    vmem = pl.BlockSpec(memory_space=VMEM)
    hbm = pl.BlockSpec(memory_space=pl.ANY)
    f32, bf16 = jnp.float32, jnp.bfloat16
    in_hbm = [
        pltpu.with_memory_space_constraint(a, pltpu.HBM)
        for a in (tokens, wq, wk, wv, wo, cosine, sine)
    ]
    tokens, wq, wk, wv, wo, cosine, sine = in_hbm
    return pl.pallas_call(
        functools.partial(layer_kernel, mp_size),
        out_shape=[VMEM((slots, share), f32)] * mp_size,
        in_specs=[smem, hbm, hbm, hbm, hbm, hbm, hbm, hbm, hbm, hbm, hbm],
        out_specs=[vmem] * mp_size,
        scratch_shapes=[
            VMEM((buffer_len, width), bf16),
            VMEM(wq.shape, bf16),
            VMEM((width, 2 * HEAD_DIM), bf16),
            VMEM(wo.shape, bf16),
            VMEM((buffer_len, HEAD_DIM), f32),
            VMEM((buffer_len, HEAD_DIM), f32),
            VMEM((ROWS, wq.shape[1]), f32),
            VMEM((ROWS, 2 * HEAD_DIM), f32),
            VMEM((ROWS, HEAD_DIM), f32),
            VMEM((buffer_len // QBLOCK, heads * QBLOCK, HEAD_DIM), bf16),
            VMEM((buffer_len, HEAD_DIM), bf16),
            VMEM((buffer_len, HEAD_DIM), bf16),
            VMEM((1, buffer_len), jnp.int32),
            VMEM((16, share), f32),
            VMEM((16, buffer_len), f32),
            VMEM((slots, width), f32),
            VMEM((1, width), bf16),
            VMEM((width,), bf16),
            pltpu.SMEM((slots,), jnp.int32),
            pltpu.SMEM((slots,), jnp.int32),
            pltpu.SemaphoreType.DMA((blocks - 1,)),
            pltpu.SemaphoreType.DMA((CHUNKS, 4)),
            pltpu.SemaphoreType.DMA((6,)),
        ],
        compiler_params=pltpu.CompilerParams(vmem_limit_bytes=LAYER_VMEM),
        name="layer",
    )(rank, starts, lengths, tokens, gain, wq, wk, wv, wo, cosine, sine)


def gram_kernel(dp_size, rank_ref, *rest):
    parts, (all_ref, gram_ref) = rest[: dp_size // 2], rest[dp_size // 2 :]
    rank = rank_ref[0]
    rows = parts[0].shape[0] // 2
    for j in range(dp_size // 2):
        for side in range(2):
            owner = rank ^ (2 * j + side)
            all_ref[pl.ds(pl.multiple_of(owner * rows, rows), rows), :] = parts[j][
                side * rows : (side + 1) * rows, :
            ]
    pooled = all_ref[...]
    gram_ref[...] = lax.dot_general(
        pooled, pooled, (((1,), (1,)), ((), ())), precision=HIGHEST,
        preferred_element_type=jnp.float32,
    )


def score_kernel(mp_size, width, episodes, rank_ref, *rest):
    grams = rest[:mp_size]
    all_ref, ids_ref, own_ref, log_ref, proto_ref, cross_s = rest[mp_size:]
    rank = rank_ref[0]
    total = all_ref.shape[0]
    own_count = log_ref.shape[0]
    classes = episodes * WAYS
    gram = grams[0][...]
    for k in range(1, mp_size):
        gram = gram + grams[k][...]
    eye = lax.broadcasted_iota(jnp.int32, (total, total), 0) == lax.broadcasted_iota(
        jnp.int32, (total, total), 1
    )
    square = jnp.sum(jnp.where(eye, gram, 0.0), axis=1, keepdims=True)
    scale = lax.rsqrt(square * (1.0 / width) + 1e-06)
    label = jnp.max(jnp.where(eye, ids_ref[...], -1), axis=1, keepdims=True)
    class_of = lax.broadcasted_iota(jnp.int32, (total, classes), 1)
    select = jnp.where(label == class_of, scale, 0.0)
    raw_protos = lax.dot_general(
        select, all_ref[...], (((0,), (0,)), ((), ())), precision=HIGHEST,
        preferred_element_type=jnp.float32,
    )
    cross = jnp.dot(gram, select, precision=HIGHEST, preferred_element_type=jnp.float32)
    norm = jnp.maximum(jnp.sum(cross * select, axis=0, keepdims=True), 0.0)
    proto_scale = lax.rsqrt(norm * (1.0 / width) + 1e-06)
    same = lax.broadcasted_iota(jnp.int32, (classes, classes), 0) == lax.broadcasted_iota(
        jnp.int32, (classes, classes), 1
    )
    proto_ref[...] = raw_protos * jnp.sum(
        jnp.where(same, proto_scale, 0.0), axis=1, keepdims=True
    )
    cross_s[...] = (
        square * scale * scale
        + norm * proto_scale * proto_scale
        - 2.0 * (scale * proto_scale) * cross
    )
    distance = cross_s[pl.ds(pl.multiple_of(rank * own_count, own_count), own_count), :]
    own_episode = own_ref[:, 0:1]
    own_query = own_ref[:, 1:2]
    picked = distance[:, :WAYS]
    for e in range(1, episodes):
        picked = jnp.where(own_episode == e, distance[:, e * WAYS : (e + 1) * WAYS], picked)
    logits = picked * (-1.0 / math.sqrt(width))
    peak = jnp.max(logits, axis=1, keepdims=True)
    shifted = logits - peak
    out = shifted - jnp.log(jnp.sum(jnp.exp(shifted), axis=1, keepdims=True))
    log_ref[...] = jnp.where(own_query == 1, out, 0.0)


def in_vmem(x):
    return pltpu.with_memory_space_constraint(x, VMEM)


def paired(size, k):
    return [(i, i ^ k) for i in range(size)]


def MP_ORDER(size):
    return range(size - 1, 0, -1)


def DP_ORDER(size):
    return range(size - 2, 0, -2)


def per_device(
    tokens, norm_gain, w_query, w_key, w_value, w_out,
    seq_starts, seq_lengths, episode_ids, class_ids, query_flags,
):
    width = tokens.shape[1]
    slots = seq_starts.shape[0]
    total = episode_ids.shape[0]
    episodes = max(1, total // (2 * WAYS))
    mp_size = lax.axis_size("mp")
    dp_size = lax.axis_size("dp")
    mp_rank = lax.axis_index("mp")
    dp_rank = lax.axis_index("dp")
    share = width // mp_size
    f32 = jnp.float32
    vmem = pl.BlockSpec(memory_space=VMEM)
    smem = pl.BlockSpec(memory_space=pltpu.SMEM)

    parts = layer_call(
        mp_size, mp_rank.reshape(1), seq_starts, seq_lengths, tokens,
        norm_gain, w_query, w_key, w_value, w_out,
    )
    pooled = parts[0]
    for k in MP_ORDER(mp_size):
        pooled = pooled + lax.ppermute(parts[k], "mp", paired(mp_size, k))

    partner = lax.ppermute(pooled, "dp", paired(dp_size, 1))
    pair = jnp.concatenate([pooled, partner], axis=0)
    gathered = {0: pair}
    for k in DP_ORDER(dp_size):
        gathered[k] = lax.ppermute(pair, "dp", paired(dp_size, k))
    everyone, gram = pl.pallas_call(
        functools.partial(gram_kernel, dp_size),
        out_shape=[VMEM((total, share), f32), VMEM((total, total), f32)],
        in_specs=[smem] + [vmem] * (dp_size // 2),
        out_specs=[vmem, vmem],
        compiler_params=pltpu.CompilerParams(vmem_limit_bytes=SMALL_VMEM),
        name="gram",
    )(dp_rank.reshape(1), *[in_vmem(gathered[k]) for k in range(0, dp_size, 2)])

    grams = [gram] + [lax.ppermute(gram, "mp", paired(mp_size, k)) for k in MP_ORDER(mp_size)]
    ids = jnp.where(query_flags == 0, episode_ids * WAYS + class_ids, -1).reshape(1, total)
    own_first = dp_rank * slots
    own = jnp.stack(
        [
            lax.dynamic_slice_in_dim(episode_ids, own_first, slots, 0),
            lax.dynamic_slice_in_dim(query_flags, own_first, slots, 0),
        ],
        axis=1,
    )
    log_probs, prototypes = pl.pallas_call(
        functools.partial(score_kernel, mp_size, width, episodes),
        out_shape=[
            jax.ShapeDtypeStruct((slots, WAYS), f32),
            jax.ShapeDtypeStruct((episodes * WAYS, share), f32),
        ],
        in_specs=[smem] + [vmem] * (mp_size + 3),
        out_specs=[vmem, vmem],
        scratch_shapes=[VMEM((total, episodes * WAYS), f32)],
        compiler_params=pltpu.CompilerParams(vmem_limit_bytes=SMALL_VMEM),
        name="score",
    )(dp_rank.reshape(1), *[in_vmem(g) for g in grams], in_vmem(everyone), ids, own)
    return log_probs, prototypes


def solution(mesh):
    placed = (
        P("dp", None), P(), P(None, "mp"), P(None, "mp"), P(None, "mp"), P("mp", None),
        P("dp"), P("dp"), P(), P(), P(),
    )
    return jax.shard_map(
        per_device,
        mesh=mesh,
        in_specs=placed,
        out_specs=(P("dp", None), P(None, "mp")),
        check_vma=False,
    )
```
